32 devices in a mesh: dp: 8 (over z, y), tensor: 4 (over x, core).
Axes of the slice: x: 2, y: 2, z: 4, core: 2. Of those that a mesh axis runs over, the one named last changes fastest.
Arguments:
- layer_input: bfloat16 [16384, 768], P(('dp', 'tensor')), may hold values from -6 to 6
- out_grad: bfloat16 [16384, 768], P(('dp', 'tensor')), may hold values from -6 to 6
- lengths: int32 [16], P('dp'), may hold values from 256 to 1024, as said below
- entry_weight: bfloat16 [768, 3, 768], P('dp', None, 'tensor'), may hold values from -0.21875 to 0.21875
- query_bias: float32 [768], replicated, may hold values from -3 to 3
- value_bias: float32 [768], replicated, may hold values from -3 to 3
- exit_weight: bfloat16 [768, 768], P('tensor', 'dp'), may hold values from -3.5 to 3.5
- exit_bias: float32 [768], replicated, may hold values from -2 to 2
- first_gain: float32 [768], replicated, may hold values from 0.5 to 1.5
- first_shift: float32 [768], replicated, may hold values from -1.5 to 1.5
- up_weight: bfloat16 [768, 3072], P('dp', 'tensor'), may hold values from -0.21875 to 0.21875
- up_bias: float32 [3072], replicated, may hold values from -3 to 3
- down_weight: bfloat16 [3072, 768], P('tensor', 'dp'), may hold values from -0.15625 to 0.15625
- down_bias: float32 [768], replicated, may hold values from -2 to 2
- second_gain: float32 [768], replicated, may hold values from 0.5 to 1.5
- second_shift: float32 [768], replicated, may hold values from -1.5 to 1.5
Outputs:
- layer_output: bfloat16 [16384, 768], P(('dp', 'tensor'))
- input_grad: float32 [16384, 768], P(('dp', 'tensor'))
- entry_grad: float32 [768, 3, 768], P('dp', None, 'tensor')
- query_bias_grad: float32 [768], replicated
- value_bias_grad: float32 [768], replicated
- exit_grad: float32 [768, 768], P('tensor', 'dp')
- exit_bias_grad: float32 [768], replicated
- first_gain_grad: float32 [768], replicated
- first_shift_grad: float32 [768], replicated
- up_grad: float32 [768, 3072], P('dp', 'tensor')
- up_bias_grad: float32 [3072], replicated
- down_grad: float32 [3072, 768], P('tensor', 'dp')
- down_bias_grad: float32 [768], replicated
- second_gain_grad: float32 [768], replicated
- second_shift_grad: float32 [768], replicated
The draws below stay inside these ranges and needn't reach their ends.
Inputs may be any that keep to these rules, and one draw needn't show every extreme that they name: `lengths`: the number of leading tokens of each sequence that are not padding; some sequence is full and some has 256.
All inputs are finite; a program needn't handle non-finite values.
Results may differ from the reference program's by a relative error of at most 0.023.
Values may be sent and summed in bfloat16 or wider, within the bound.
A program may use at most 128 MiB of HBM per device.

```python
import math
import jax
import jax.numpy as jnp
from jax import lax

D = 768
HEADS = 12
HD = 64
FF = 3072
LEN = 1024
SEQS = 16
TOKENS = 16384
N_TENSOR = 4


def draw_lengths(key, part):
    values = jax.random.randint(key, (SEQS,), LEN // 4, LEN + 1)
    values = values.at[0].set(LEN)
    values = values.at[SEQS - 1].set(LEN // 4)
    return values.astype(jnp.int32)


def spiked(entries, stream_key, source, target, blocks, factor):
    def block_of(axis_at):
        return (jnp.arange(entries.shape[axis_at]) // (entries.shape[axis_at] // blocks)).reshape((-1,) + (1,) * (entries.ndim - 1 - axis_at))

    first = jax.random.permutation(stream_key, blocks)[block_of(target)]
    second = (block_of(target) + blocks // 2) % blocks
    return jnp.where((block_of(source) == first) | (block_of(source) == second), factor * entries, entries)


def level_of(key, shape, cuts, smallest, largest):
    def one(dim, blocks):
        heights = jax.random.uniform(jax.random.fold_in(jax.random.fold_in(key, 6), dim), (blocks,), jnp.float32, smallest / len(cuts), largest / len(cuts))
        return jnp.repeat(jnp.exp(heights), shape[dim] // blocks).reshape((-1,) + (1,) * (len(shape) - dim - 1))

    factor_of = one(*cuts[0])
    for cut in cuts[1:]:
        factor_of = factor_of * one(*cut)
    return factor_of


def noise(key, dims, scale, reach, cuts=(), held_as=jnp.bfloat16):
    loudness = level_of(key, dims, cuts, -0.22, 0.18) if cuts else 1.0
    entries = jax.random.normal(key, dims, jnp.float32) * scale * loudness
    return jnp.minimum(jnp.maximum(entries, -reach), reach).astype(held_as)


def gaussian_with(own_key, extent, scale, most, cuts, heavy, dtype=jnp.bfloat16):
    array = scale * jax.random.normal(own_key, extent, jnp.float32)
    if cuts:
        array = array * level_of(own_key, extent, cuts, -0.22, 0.18)
    return jnp.clip(spiked(array, jax.random.fold_in(own_key, 3), *heavy), -most, most).astype(dtype)


def setup_inputs(seed: int = 0) -> dict:
    key_list = jax.random.split(jax.random.key(seed), 17)
    return {
        "layer_input": gaussian_with(key_list[0], (TOKENS, D), 1.0, 6.0, ((0, 32),), (0, 1, 32, 2.75)),
        "out_grad": gaussian_with(key_list[1], (TOKENS, D), 1.0, 6.0, ((0, 32),), (0, 1, 32, 2.75)),
        "lengths": draw_lengths(jax.random.fold_in(key_list[16], 71), 0),
        "entry_weight": noise(key_list[3], (D, 3, D), D ** -0.5, 0.21875, ((0, 8), (2, 4))),
        "query_bias": noise(key_list[4], (D,), 0.5, 3.0, (), jnp.float32),
        "value_bias": noise(key_list[5], (D,), 0.5, 3.0, (), jnp.float32),
        "exit_weight": noise(key_list[6], (D, D), (max(4 * D // LEN, 1)) ** -0.5, 3.5, ((0, 4), (1, 8))),
        "exit_bias": noise(key_list[7], (D,), 0.3, 2.0, (), jnp.float32),
        "first_gain": jnp.clip(1.0 + 0.1 * jax.random.normal(key_list[8], (D,), jnp.float32), 0.5, 1.5),
        "first_shift": noise(key_list[9], (D,), 0.2, 1.5, (), jnp.float32),
        "up_weight": noise(key_list[10], (D, FF), D ** -0.5, 0.21875, ((0, 8), (1, 4))),
        "up_bias": noise(key_list[11], (FF,), 0.5, 3.0, (), jnp.float32),
        "down_weight": noise(key_list[12], (FF, D), (FF // 2) ** -0.5, 0.15625, ((0, 4), (1, 8))),
        "down_bias": noise(key_list[13], (D,), 0.3, 2.0, (), jnp.float32),
        "second_gain": jnp.clip(1.0 + 0.1 * jax.random.normal(key_list[14], (D,), jnp.float32), 0.5, 1.5),
        "second_shift": noise(key_list[15], (D,), 0.2, 1.5, (), jnp.float32),
    }


@jax.custom_vjp
def low(v):
    return lax.optimization_barrier(v.astype(jnp.bfloat16)).astype(jnp.float32)

@jax.custom_vjp
def low_back(v):
    return v

def low_keep(v):
    return (low(v), None)

def low_pass(kept, grad):
    return (grad,)

def back_keep(v):
    return (v, None)

def back_low(kept, grad):
    return (low(grad),)
low.defvjp(low_keep, low_pass)
low_back.defvjp(back_keep, back_low)
EPSILON = 1e-12
HIGHEST = lax.Precision.HIGHEST

def layer_norm(rows, gain, shift):
    center = rows - lax.optimization_barrier(jnp.mean(rows, axis=-1, keepdims=True))
    spread = lax.optimization_barrier(jnp.mean(center * center, axis=-1, keepdims=True))
    return center * lax.rsqrt(spread + EPSILON) * gain + shift

def attend(item):
    queries, keys, values, length = item
    scale = 1.0 / math.sqrt(HD)
    scores = jnp.einsum('qhd,khd->hqk', queries, keys, precision=HIGHEST, preferred_element_type=jnp.float32) * scale
    scores = low_back(scores)
    valid = jnp.arange(LEN).astype(jnp.int32) < length.astype(jnp.int32)
    scores = jnp.where(valid[None, None, :], scores, -1e+30)
    probs = low(jax.nn.softmax(scores, axis=-1))
    return jnp.einsum('hqk,khd->qhd', probs, values, precision=HIGHEST, preferred_element_type=jnp.float32)

def split_sum(left, right, parts):
    inner = left.shape[1] // parts
    total = jnp.zeros((left.shape[0], right.shape[1]), jnp.float32)
    for index in range(parts):
        piece = jnp.dot(left[:, index * inner:(index + 1) * inner], right[index * inner:(index + 1) * inner], precision=HIGHEST, preferred_element_type=jnp.float32)
        total = total + low(piece)
    return total

def forward(block_in, block_len, entry_weight, query_bias, value_bias, exit_weight, exit_bias, first_gain, first_shift, up_weight, up_bias, down_weight, down_bias, second_gain, second_shift):
    group = block_in.shape[0]
    rows = block_in.reshape(group * LEN, D)
    local_width = D // N_TENSOR
    pieces = []
    for index in range(N_TENSOR):
        columns = entry_weight[:, :, index * local_width:(index + 1) * local_width].reshape(D, 3 * local_width)
        piece = jnp.dot(low_back(rows), columns, precision=HIGHEST, preferred_element_type=jnp.float32)
        pieces.append(piece.reshape(group * LEN, 3, local_width))
    mixed = jnp.concatenate(pieces, axis=2)
    offsets = jnp.stack([query_bias, jnp.zeros_like(query_bias), value_bias])
    mixed = low_back(low(mixed + offsets))
    queries = mixed[:, 0].reshape(group, LEN, HEADS, HD)
    keys = mixed[:, 1].reshape(group, LEN, HEADS, HD)
    values = mixed[:, 2].reshape(group, LEN, HEADS, HD)
    context = lax.map(jax.checkpoint(attend), (queries, keys, values, block_len))
    context = low_back(low(context.reshape(group * LEN, D)))
    attended = low_back(split_sum(context, exit_weight, N_TENSOR))
    normed = low(layer_norm(rows + attended + exit_bias, first_gain, first_shift))
    local_hidden = FF // N_TENSOR
    upper_pieces = []
    for index in range(N_TENSOR):
        upper_pieces.append(jnp.dot(low_back(normed), up_weight[:, index * local_hidden:(index + 1) * local_hidden], precision=HIGHEST, preferred_element_type=jnp.float32))
    upper = low_back(jnp.concatenate(upper_pieces, axis=1) + up_bias)
    active = low(jax.nn.gelu(upper, approximate=False))
    lowered = low_back(split_sum(active, down_weight, N_TENSOR))
    return layer_norm(normed + lowered + down_bias, second_gain, second_shift)

def reference(layer_input, out_grad, lengths, entry_weight, query_bias, value_bias, exit_weight, exit_bias, first_gain, first_shift, up_weight, up_bias, down_weight, down_bias, second_gain, second_shift):
    params = tuple((item.astype(jnp.float32) for item in (entry_weight, query_bias, value_bias, exit_weight, exit_bias, first_gain, first_shift, up_weight, up_bias, down_weight, down_bias, second_gain, second_shift)))
    group = math.gcd(SEQS, 4)
    inputs = layer_input.astype(jnp.float32).reshape(SEQS // group, group, LEN, D)
    cotangents = out_grad.astype(jnp.float32).reshape(SEQS // group, group * LEN, D)
    spans = lengths.astype(jnp.int32).reshape(SEQS // group, group)

    def one_group(totals, item):
        block_in, block_grad, block_len = item

        def apply(block, *weights):
            return forward(block, block_len, *weights)
        result, pullback = jax.vjp(apply, block_in, *params)
        grads = pullback(block_grad)
        totals = tuple((left + right for left, right in zip(totals, grads[1:])))
        return (totals, (result.astype(jnp.bfloat16), grads[0].reshape(group * LEN, D)))
    zeros = tuple((jnp.zeros_like(item) for item in params))
    totals, (outputs, input_grads) = lax.scan(one_group, zeros, (inputs, cotangents, spans))
    return (outputs.reshape(TOKENS, D), input_grads.reshape(TOKENS, D), totals[0], totals[1], totals[2], totals[3], totals[4], totals[5], totals[6], totals[7], totals[8], totals[9], totals[10], totals[11], totals[12])
```

```python
import math

import jax
import jax.numpy as jnp
from jax import lax
from jax.experimental import pallas as pl
from jax.experimental.pallas import tpu as pltpu
from jax.sharding import PartitionSpec as P


HD = 64
LEN = 1024
EPSILON = 1e-12
NEG_FILL = -1e30
AXES = ("dp", "tensor")
F32 = jnp.float32
BF16 = jnp.bfloat16
ROWS_DIMS = (((0,), (0,)), ((), ()))
LAST_DIMS = (((1,), (1,)), ((), ()))


def across(left, right):
    return lax.dot_general(left, right, ROWS_DIMS, preferred_element_type=F32)


def against(left, right):
    return lax.dot_general(left, right, LAST_DIMS, preferred_element_type=F32)


def plain(left, right):
    return jnp.dot(left, right, preferred_element_type=F32)


def norm_parts(rows):
    center = rows - jnp.mean(rows, axis=-1, keepdims=True)
    spread = jnp.mean(center * center, axis=-1, keepdims=True)
    inverse = lax.rsqrt(spread + EPSILON)
    return center * inverse, inverse


def norm_back(grad, gain, unit, inverse):
    scaled = grad * gain
    return inverse * (
        scaled
        - jnp.mean(scaled, axis=-1, keepdims=True)
        - unit * jnp.mean(scaled * unit, axis=-1, keepdims=True)
    )


def attend_kernel(length_ref, q_ref, k_ref, v_ref, context_ref, stat_ref, *, scale):
    length = length_ref[0]
    block = q_ref.shape[0]
    valid = lax.broadcasted_iota(jnp.int32, (1, k_ref.shape[0]), 1) < length
    lane = lax.broadcasted_iota(jnp.int32, (block, 128), 1)
    stats = jnp.zeros((block, 128), F32)
    pieces = []
    for head in range(2):
        cols = slice(head * HD, (head + 1) * HD)
        scores = lax.dot_general(q_ref[:, cols], k_ref[:, cols], LAST_DIMS, preferred_element_type=F32) * scale
        scores = jnp.where(valid, scores, NEG_FILL)
        row_max = jnp.max(scores, axis=-1, keepdims=True)
        weights = jnp.exp(scores - row_max)
        total = jnp.sum(weights, axis=-1, keepdims=True)
        mixed = jnp.dot(weights.astype(BF16), v_ref[:, cols], preferred_element_type=F32)
        pieces.append(mixed / total)
        stats = jnp.where(lane == head, row_max + jnp.log(total), stats)
    context_ref[...] = jnp.concatenate(pieces, axis=1).astype(BF16)
    stat_ref[...] = jnp.transpose(stats)[:8]


def attend(mixed, length, heads, scale):
    rows = mixed.shape[0]
    pairs = heads // 2
    block = min(512, rows)
    return pl.pallas_call(
        lambda *refs: attend_kernel(*refs, scale=scale),
        out_shape=(
            jax.ShapeDtypeStruct((rows, heads * HD), BF16),
            jax.ShapeDtypeStruct((pairs * 8, rows), F32),
        ),
        grid_spec=pltpu.PrefetchScalarGridSpec(
            num_scalar_prefetch=1,
            grid=(pairs, rows // block),
            in_specs=[
                pl.BlockSpec((block, 128), lambda p, b, n: (b, p)),
                pl.BlockSpec((rows, 128), lambda p, b, n: (0, pairs + p)),
                pl.BlockSpec((rows, 128), lambda p, b, n: (0, 2 * pairs + p)),
            ],
            out_specs=(
                pl.BlockSpec((block, 128), lambda p, b, n: (b, p)),
                pl.BlockSpec((8, block), lambda p, b, n: (p, b)),
            ),
        ),
        cost_estimate=pl.CostEstimate(
            flops=16 * heads * rows * rows * HD, bytes_accessed=8 * rows * heads * HD, transcendentals=heads * rows * rows
        ),
        name="attend",
    )(length, mixed, mixed, mixed)


def attend_back_kernel(
    length_ref, q_ref, k_ref, v_ref, g_ref, stat_ref, dq_ref, dk_ref, dv_ref, key_total, value_total, *, scale
):
    step = pl.program_id(1)
    length = length_ref[0]
    rows = k_ref.shape[0]
    valid = lax.broadcasted_iota(jnp.int32, (rows, 1), 0) < length

    @pl.when(step == 0)
    def _():
        key_total[...] = jnp.zeros_like(key_total)
        value_total[...] = jnp.zeros_like(value_total)

    turned = jnp.transpose(k_ref[...])
    queries = []
    for head in range(2):
        cols = slice(head * HD, (head + 1) * HD)
        q, k, v, g = q_ref[:, cols], k_ref[:, cols], v_ref[:, cols], g_ref[:, cols]
        scores = lax.dot_general(k, q, LAST_DIMS, preferred_element_type=F32) * scale
        scores = jnp.where(valid, scores, NEG_FILL)
        probs = jnp.exp(scores - stat_ref[head : head + 1, :])
        prob_grad = lax.dot_general(v, g, LAST_DIMS, preferred_element_type=F32)
        delta = jnp.sum(probs * prob_grad, axis=0, keepdims=True)
        score_grad = (probs * (prob_grad - delta)).astype(BF16)
        value_total[:, cols] += jnp.dot(probs.astype(BF16), g, preferred_element_type=F32)
        key_total[:, cols] += jnp.dot(score_grad, q, preferred_element_type=F32)
        queries.append(jnp.dot(turned[cols, :], score_grad, preferred_element_type=F32))
    dq_ref[...] = (jnp.transpose(jnp.concatenate(queries, axis=0)) * scale).astype(BF16)

    @pl.when(step == pl.num_programs(1) - 1)
    def _():
        dk_ref[...] = (key_total[...] * scale).astype(BF16)
        dv_ref[...] = value_total[...].astype(BF16)


def attend_back(mixed, context_grad, stats, length, heads, scale):
    rows = mixed.shape[0]
    pairs = heads // 2
    block = min(512, rows)
    piece = jax.ShapeDtypeStruct((rows, heads * HD), BF16)
    return pl.pallas_call(
        lambda *refs: attend_back_kernel(*refs, scale=scale),
        out_shape=(piece, piece, piece),
        grid_spec=pltpu.PrefetchScalarGridSpec(
            num_scalar_prefetch=1,
            grid=(pairs, rows // block),
            in_specs=[
                pl.BlockSpec((block, 128), lambda p, b, n: (b, p)),
                pl.BlockSpec((rows, 128), lambda p, b, n: (0, pairs + p)),
                pl.BlockSpec((rows, 128), lambda p, b, n: (0, 2 * pairs + p)),
                pl.BlockSpec((block, 128), lambda p, b, n: (b, p)),
                pl.BlockSpec((8, block), lambda p, b, n: (p, b)),
            ],
            out_specs=(
                pl.BlockSpec((block, 128), lambda p, b, n: (b, p)),
                pl.BlockSpec((rows, 128), lambda p, b, n: (0, p)),
                pl.BlockSpec((rows, 128), lambda p, b, n: (0, p)),
            ),
            scratch_shapes=[pltpu.VMEM((rows, 128), F32), pltpu.VMEM((rows, 128), F32)],
        ),
        cost_estimate=pl.CostEstimate(
            flops=40 * heads * rows * rows * HD, bytes_accessed=16 * rows * heads * HD, transcendentals=heads * rows * rows
        ),
        name="attend_back",
    )(length, mixed, mixed, mixed, context_grad, stats)


class Places:
    def __init__(self, dp, tensor):
        self.dp, self.tensor = dp, tensor
        self.deep_bits = (dp // 2).bit_length() - 1
        d, t = lax.axis_index("dp"), lax.axis_index("tensor")
        self.core, self.side, self.near, self.deep = t % 2, t // 2, d % 2, d // 2

    def swap(self, value, dp_mask, tensor_mask):
        pairs = [
            (d * self.tensor + t, (d ^ dp_mask) * self.tensor + (t ^ tensor_mask))
            for d in range(self.dp)
            for t in range(self.tensor)
        ]
        return lax.ppermute(value, AXES, pairs)

    def swap_core(self, value):
        return self.swap(value, 0, 1)

    def swap_side(self, value):
        return self.swap(value, 0, 2)

    def swap_near(self, value):
        return self.swap(value, 1, 0)

    def swap_deep(self, value, bit):
        return self.swap(value, 2 << bit, 0)

    def deep_bit(self, bit):
        return (self.deep >> bit) % 2


def ordered(index, own, other, axis):
    first = jnp.where(index == 0, own, other)
    second = jnp.where(index == 0, other, own)
    return jnp.stack([first, second], axis=axis)


def pick(index, stacked, axis):
    return lax.dynamic_index_in_dim(stacked, index, axis, keepdims=False)


def gather_weight(at, shard):
    rows, cols = shard.shape
    whole = shard[None]
    for bit in reversed(range(at.deep_bits)):
        got = at.swap_deep(whole, bit)
        whole = ordered(at.deep_bit(bit), whole, got, 1).reshape(-1, rows, cols)
        if bit == at.deep_bits - 1:
            first_done = whole
    upper, lower = whole[:, : rows // 2], whole[:, rows // 2 :]
    got_upper, got_lower = at.swap_side(upper), at.swap_near(lower)
    upper = ordered(at.side, upper, got_upper, 0)
    lower = ordered(at.near, lower, got_lower, 1)
    got_upper, got_lower = at.swap_near(upper), at.swap_side(lower)
    upper = ordered(at.near, upper, got_upper, 2)
    lower = ordered(at.side, lower, got_lower, 0)
    return jnp.concatenate([upper, lower], axis=3).reshape(2, at.dp * rows, cols), first_done


def scatter_grad(at, parts):
    cols = parts[0].shape[1]
    rows = parts[0].shape[0] // at.dp
    stacked = jnp.stack([p.reshape(at.dp // 2, 2, 2, rows // 2, cols) for p in parts])
    upper, lower = stacked[:, :, :, 0], stacked[:, :, :, 1]
    got_upper = at.swap_near(pick(1 - at.near, upper, 2))
    got_lower = at.swap_side(pick(1 - at.side, lower, 0))
    upper = pick(at.near, upper, 2).astype(F32) + got_upper.astype(F32)
    lower = pick(at.side, lower, 0).astype(F32) + got_lower.astype(F32)
    got_upper = at.swap_side(pick(1 - at.side, upper, 0).astype(BF16))
    got_lower = at.swap_near(pick(1 - at.near, lower, 1).astype(BF16))
    upper = pick(at.side, upper, 0) + got_upper.astype(F32)
    lower = pick(at.near, lower, 1) + got_lower.astype(F32)
    total = jnp.concatenate([upper, lower], axis=1)
    for bit in range(at.deep_bits):
        total = total.reshape(-1, 2, rows, cols)
        got = at.swap_deep(pick(1 - at.deep_bit(bit), total, 1).astype(BF16), bit)
        total = pick(at.deep_bit(bit), total, 1) + got.astype(F32)
    return total.reshape(rows, cols)


def body(
    layer_input,
    out_grad,
    lengths,
    entry_weight,
    query_bias,
    value_bias,
    exit_weight,
    exit_bias,
    first_gain,
    first_shift,
    up_weight,
    up_bias,
    down_weight,
    down_bias,
    second_gain,
    second_shift,
):
    at = Places(lax.axis_size("dp"), lax.axis_size("tensor"))
    own, width = layer_input.shape
    part = entry_weight.shape[2]
    hidden = up_weight.shape[1]
    shard_rows = entry_weight.shape[0]
    heads = 2 * part // HD
    scale = 1.0 / math.sqrt(HD)

    def mine(vector):
        pieces = vector.reshape(2, 2, vector.shape[0] // 4)
        return pick(at.core, pieces, 1).reshape(-1)

    def placed(local):
        pieces = local.reshape(2, 1, local.shape[0] // 2)
        empty = jnp.zeros((2, 2, local.shape[0] // 2), F32)
        return lax.dynamic_update_slice(empty, pieces, (0, at.core, 0)).reshape(-1)

    def half(rows, index):
        return lax.dynamic_slice_in_dim(rows, index * own, own, 0)

    def both(rows):
        return ordered(at.core, rows, at.swap_core(rows), 0).reshape(2 * own, rows.shape[1])

    def shared_sum(rows, weight):
        far = at.swap_core(against(half(rows, 1 - at.core), weight).astype(BF16))
        return against(half(rows, at.core), weight) + far.astype(F32)

    packed = jnp.concatenate([entry_weight.reshape(shard_rows, 3 * part), exit_weight.T], axis=1)
    packed_full, mark = gather_weight(at, packed)
    up_shard, mark = lax.optimization_barrier((up_weight, mark))
    up_parts, mark = gather_weight(at, up_shard)
    down_shard, mark = lax.optimization_barrier((down_weight.T, mark))
    down_parts, mark = gather_weight(at, down_shard)
    entry_matrix = (
        packed_full[:, :, : 3 * part].reshape(2, width, 3, part).transpose(1, 2, 0, 3).reshape(width, 6 * part)
    )
    exit_matrix = packed_full[:, :, 3 * part :].transpose(1, 0, 2).reshape(width, 2 * part)
    up_matrix = up_parts.transpose(1, 0, 2).reshape(width, 2 * hidden)
    down_matrix = down_parts.transpose(1, 0, 2).reshape(width, 2 * hidden)

    length = lax.dynamic_slice_in_dim(lengths, at.side, 1)
    rows_all = both(layer_input)
    query_local = mine(query_bias)
    offsets = jnp.concatenate([query_local, jnp.zeros_like(query_local), mine(value_bias)])
    mixed = (plain(rows_all, entry_matrix) + offsets).astype(BF16)
    context, stats = attend(mixed, length, heads, scale)
    attended = shared_sum(context, exit_matrix)
    first_sum = layer_input.astype(F32) + attended + exit_bias
    first_unit, first_inverse = norm_parts(first_sum)
    normed = (first_unit * first_gain + first_shift).astype(BF16)

    normed_all = both(normed)
    upper = plain(normed_all, up_matrix) + mine(up_bias)
    active_full, gelu_pull = jax.vjp(lambda u: jax.nn.gelu(u, approximate=False), upper)
    active = active_full.astype(BF16)
    lowered = shared_sum(active, down_matrix)
    second_sum = normed.astype(F32) + lowered + down_bias
    second_unit, second_inverse = norm_parts(second_sum)
    layer_output = (second_unit * second_gain + second_shift).astype(BF16)

    grad = out_grad.astype(F32)
    second_grad = norm_back(grad, second_gain, second_unit, second_inverse)
    second_gain_grad = jnp.sum(grad * second_unit, axis=0)
    second_shift_grad = jnp.sum(grad, axis=0)
    down_bias_grad = jnp.sum(second_grad, axis=0)
    lowered_all = both(second_grad.astype(BF16))
    upper_grad = gelu_pull(plain(lowered_all, down_matrix))[0].astype(BF16)
    down_partial = across(lowered_all, active).astype(BF16)
    down_grad = scatter_grad(at, [down_partial[:, :hidden], down_partial[:, hidden:]])
    up_bias_local = jnp.sum(upper_grad.astype(F32), axis=0)
    normed_grad = second_grad + shared_sum(upper_grad, up_matrix)
    up_partial = across(normed_all, upper_grad).astype(BF16)
    up_grad = scatter_grad(at, [up_partial[:, :hidden], up_partial[:, hidden:]])

    first_grad = norm_back(normed_grad, first_gain, first_unit, first_inverse)
    first_gain_grad = jnp.sum(normed_grad * first_unit, axis=0)
    first_shift_grad = jnp.sum(normed_grad, axis=0)
    exit_bias_grad = jnp.sum(first_grad, axis=0)
    attended_all = both(first_grad.astype(BF16))
    context_grad = plain(attended_all, exit_matrix).astype(BF16)
    exit_partial = across(attended_all, context).astype(BF16)
    query_grad, key_grad, value_grad = attend_back(mixed, context_grad, stats, length, heads, scale)
    query_bias_local = jnp.sum(query_grad.astype(F32), axis=0)
    value_bias_local = jnp.sum(value_grad.astype(F32), axis=0)
    mixed_grad = jnp.concatenate([query_grad, key_grad, value_grad], axis=1)
    entry_partial = across(rows_all, mixed_grad).astype(BF16)
    packed_parts = [
        jnp.concatenate(
            [entry_partial[:, (2 * k + s) * part : (2 * k + s + 1) * part] for k in range(3)]
            + [exit_partial[:, s * part : (s + 1) * part]],
            axis=1,
        )
        for s in range(2)
    ]
    packed_grad = scatter_grad(at, packed_parts)
    input_grad = first_grad + shared_sum(mixed_grad, entry_matrix)

    vectors = [
        placed(query_bias_local),
        placed(value_bias_local),
        exit_bias_grad,
        first_gain_grad,
        first_shift_grad,
        placed(up_bias_local),
        down_bias_grad,
        second_gain_grad,
        second_shift_grad,
    ]
    sizes = [v.shape[0] for v in vectors]
    total = jnp.concatenate(vectors).reshape(-1, 128)
    total = total + at.swap_core(total)
    total = total + at.swap_side(total)
    total = total + at.swap_near(total)
    for bit in range(at.deep_bits):
        total = total + at.swap_deep(total, bit)
    total = total.reshape(-1)
    sums = []
    start = 0
    for size in sizes:
        sums.append(total[start : start + size])
        start += size

    return (
        layer_output,
        input_grad,
        packed_grad[:, : 3 * part].reshape(shard_rows, 3, part),
        sums[0],
        sums[1],
        packed_grad[:, 3 * part :].T,
        sums[2],
        sums[3],
        sums[4],
        up_grad,
        sums[5],
        down_grad.T,
        sums[6],
        sums[7],
        sums[8],
    )


def solution(mesh):
    rows = P(("dp", "tensor"), None)
    return jax.shard_map(
        body,
        mesh=mesh,
        in_specs=(
            rows,
            rows,
            P("dp"),
            P("dp", None, "tensor"),
            P(),
            P(),
            P("tensor", "dp"),
            P(),
            P(),
            P(),
            P("dp", "tensor"),
            P(),
            P("tensor", "dp"),
            P(),
            P(),
            P(),
        ),
        out_specs=(
            rows,
            rows,
            P("dp", None, "tensor"),
            P(),
            P(),
            P("tensor", "dp"),
            P(),
            P(),
            P(),
            P("dp", "tensor"),
            P(),
            P("tensor", "dp"),
            P(),
            P(),
            P(),
        ),
        check_vma=False,
    )
```

```python
import math

import jax
import jax.numpy as jnp
from jax import lax
from jax.experimental import pallas as pl
from jax.experimental.pallas import tpu as pltpu
from jax.sharding import PartitionSpec as P


HD = 64
LEN = 1024
EPSILON = 1e-12
NEG_FILL = -1e30
AXES = ("dp", "tensor")
F32 = jnp.float32
BF16 = jnp.bfloat16
ROWS_DIMS = (((0,), (0,)), ((), ()))
LAST_DIMS = (((1,), (1,)), ((), ()))


def across(left, right):
    return lax.dot_general(left, right, ROWS_DIMS, preferred_element_type=F32)


def against(left, right):
    return lax.dot_general(left, right, LAST_DIMS, preferred_element_type=F32)


def plain(left, right):
    return jnp.dot(left, right, preferred_element_type=F32)


def norm_parts(rows):
    center = rows - jnp.mean(rows, axis=-1, keepdims=True)
    spread = jnp.mean(center * center, axis=-1, keepdims=True)
    inverse = lax.rsqrt(spread + EPSILON)
    return center * inverse, inverse


def norm_back(grad, gain, unit, inverse):
    scaled = grad * gain
    return inverse * (
        scaled
        - jnp.mean(scaled, axis=-1, keepdims=True)
        - unit * jnp.mean(scaled * unit, axis=-1, keepdims=True)
    )


def attend_kernel(length_ref, q_ref, all_ref, context_ref, stat_ref, *, scale, heads):
    length = length_ref[0]
    block = q_ref.shape[0]
    part = heads * HD
    valid = lax.broadcasted_iota(jnp.int32, (1, all_ref.shape[0]), 1) < length
    lane = lax.broadcasted_iota(jnp.int32, (block, 128), 1)
    stats = jnp.zeros((block, 128), F32)
    pieces = []
    for head in range(heads):
        q = q_ref[:, head * HD : (head + 1) * HD]
        k = all_ref[:, part + head * HD : part + (head + 1) * HD]
        v = all_ref[:, 2 * part + head * HD : 2 * part + (head + 1) * HD]
        scores = lax.dot_general(q, k, LAST_DIMS, preferred_element_type=F32) * scale
        scores = jnp.where(valid, scores, NEG_FILL)
        row_max = jnp.max(scores, axis=-1, keepdims=True)
        weights = jnp.exp(scores - row_max)
        total = jnp.sum(weights, axis=-1, keepdims=True)
        mixed = jnp.dot(weights.astype(BF16), v, preferred_element_type=F32)
        pieces.append(mixed / total)
        stats = jnp.where(lane == head, row_max + jnp.log(total), stats)
    context_ref[...] = jnp.concatenate(pieces, axis=1).astype(BF16)
    stat_ref[...] = jnp.transpose(stats)[:8]


def attend(mixed, length, heads, scale):
    rows, cols = mixed.shape
    block = min(512, rows)
    return pl.pallas_call(
        lambda *refs: attend_kernel(*refs, scale=scale, heads=heads),
        out_shape=(
            jax.ShapeDtypeStruct((rows, heads * HD), BF16),
            jax.ShapeDtypeStruct((8, rows), F32),
        ),
        grid_spec=pltpu.PrefetchScalarGridSpec(
            num_scalar_prefetch=1,
            grid=(rows // block,),
            in_specs=[
                pl.BlockSpec((block, cols), lambda b, n: (b, 0)),
                pl.BlockSpec((rows, cols), lambda b, n: (0, 0)),
            ],
            out_specs=(
                pl.BlockSpec((block, heads * HD), lambda b, n: (b, 0)),
                pl.BlockSpec((8, block), lambda b, n: (0, b)),
            ),
        ),
        cost_estimate=pl.CostEstimate(
            flops=16 * heads * rows * rows * HD, bytes_accessed=8 * rows * heads * HD, transcendentals=heads * rows * rows
        ),
        name="attend",
    )(length, mixed, mixed)


def attend_back_kernel(
    length_ref, q_ref, all_ref, g_ref, stat_ref, out_ref, key_total, value_total, *, scale, heads
):
    step = pl.program_id(0)
    length = length_ref[0]
    block = q_ref.shape[0]
    rows = all_ref.shape[0]
    part = heads * HD
    valid = lax.broadcasted_iota(jnp.int32, (rows, 1), 0) < length

    @pl.when(step == 0)
    def _():
        key_total[...] = jnp.zeros_like(key_total)
        value_total[...] = jnp.zeros_like(value_total)

    queries = []
    for head in range(heads):
        cols = slice(head * HD, (head + 1) * HD)
        q, g = q_ref[:, cols], g_ref[:, cols]
        k = all_ref[:, part + head * HD : part + (head + 1) * HD]
        v = all_ref[:, 2 * part + head * HD : 2 * part + (head + 1) * HD]
        scores = lax.dot_general(k, q, LAST_DIMS, preferred_element_type=F32) * scale
        scores = jnp.where(valid, scores, NEG_FILL)
        probs = jnp.exp(scores - stat_ref[head : head + 1, :])
        prob_grad = lax.dot_general(v, g, LAST_DIMS, preferred_element_type=F32)
        delta = jnp.sum(probs * prob_grad, axis=0, keepdims=True)
        score_grad = (probs * (prob_grad - delta)).astype(BF16)
        value_total[:, cols] += jnp.dot(probs.astype(BF16), g, preferred_element_type=F32)
        key_total[:, cols] += jnp.dot(score_grad, q, preferred_element_type=F32)
        turned = jnp.dot(jnp.transpose(k), score_grad, preferred_element_type=F32)
        queries.append(jnp.transpose(turned) * scale)
    start = pl.multiple_of(step * block, block)
    out_ref[pl.ds(start, block), :part] = jnp.concatenate(queries, axis=1).astype(BF16)

    @pl.when(step == pl.num_programs(0) - 1)
    def _():
        out_ref[:, part : 2 * part] = (key_total[...] * scale).astype(BF16)
        out_ref[:, 2 * part :] = value_total[...].astype(BF16)


def attend_back(mixed, context_grad, stats, length, heads, scale):
    rows, cols = mixed.shape
    block = min(512, rows)
    part = heads * HD
    return pl.pallas_call(
        lambda *refs: attend_back_kernel(*refs, scale=scale, heads=heads),
        out_shape=jax.ShapeDtypeStruct((rows, cols), BF16),
        grid_spec=pltpu.PrefetchScalarGridSpec(
            num_scalar_prefetch=1,
            grid=(rows // block,),
            in_specs=[
                pl.BlockSpec((block, cols), lambda b, n: (b, 0)),
                pl.BlockSpec((rows, cols), lambda b, n: (0, 0)),
                pl.BlockSpec((block, part), lambda b, n: (b, 0)),
                pl.BlockSpec((8, block), lambda b, n: (0, b)),
            ],
            out_specs=pl.BlockSpec((rows, cols), lambda b, n: (0, 0)),
            scratch_shapes=[pltpu.VMEM((rows, part), F32), pltpu.VMEM((rows, part), F32)],
        ),
        cost_estimate=pl.CostEstimate(
            flops=40 * heads * rows * rows * HD, bytes_accessed=16 * rows * heads * HD, transcendentals=heads * rows * rows
        ),
        name="attend_back",
    )(length, mixed, mixed, context_grad, stats)


class Places:
    def __init__(self, dp, tensor):
        self.dp, self.tensor = dp, tensor
        self.deep_bits = (dp // 2).bit_length() - 1
        d, t = lax.axis_index("dp"), lax.axis_index("tensor")
        self.core, self.side, self.near, self.deep = t % 2, t // 2, d % 2, d // 2

    def swap(self, value, dp_mask, tensor_mask):
        pairs = [
            (d * self.tensor + t, (d ^ dp_mask) * self.tensor + (t ^ tensor_mask))
            for d in range(self.dp)
            for t in range(self.tensor)
        ]
        return lax.ppermute(value, AXES, pairs)

    def swap_core(self, value):
        return self.swap(value, 0, 1)

    def swap_side(self, value):
        return self.swap(value, 0, 2)

    def swap_near(self, value):
        return self.swap(value, 1, 0)

    def swap_deep(self, value, bit):
        return self.swap(value, 2 << bit, 0)

    def deep_bit(self, bit):
        return (self.deep >> bit) % 2


def ordered(index, own, other, axis):
    first = jnp.where(index == 0, own, other)
    second = jnp.where(index == 0, other, own)
    return jnp.stack([first, second], axis=axis)


def pick(index, stacked, axis):
    return lax.dynamic_index_in_dim(stacked, index, axis, keepdims=False)


def gather_kernel(packed_ref, up_ref, down_ref, packed_out, up_out, down_out, local_sem, send, recv, *, deep_count):
    d, t = lax.axis_index("dp"), lax.axis_index("tensor")
    core, side, near, deep = t % 2, t // 2, d % 2, d // 2
    half, cols = packed_out.shape[4], packed_out.shape[5]
    shards = (packed_ref, up_ref, down_ref)
    outs = (packed_out, up_out, down_out)
    other_side = {"dp": d, "tensor": (1 - side) * 2 + core}
    other_near = {"dp": deep * 2 + 1 - near, "tensor": t}

    def deep_peer(step):
        return {"dp": lax.rem(deep + step, deep_count) * 2 + near, "tensor": t}

    def spot(w, sides, deeps, nears, halves):
        if w == 0:
            return outs[w].at[sides, deeps, nears, halves]
        columns = pl.ds(0, 2 * cols) if isinstance(sides, slice) else pl.ds(pl.multiple_of(sides * cols, cols), cols)
        return outs[w].at[deeps, nears, halves, :, columns]

    def remote(source, target, w, slot, device):
        return pltpu.make_async_remote_copy(
            src_ref=source, dst_ref=target, send_sem=send.at[w, slot], recv_sem=recv.at[w, slot],
            device_id=device, device_id_type=pl.DeviceIdType.MESH,
        )

    every = slice(None)
    first = deep_count - 1

    def deep_copies(w):
        return [remote(shards[w], spot(w, side, deep, near, every), w, k - 1, deep_peer(k)) for k in range(1, deep_count)]

    def middle_copies(w):
        upper, lower = spot(w, side, every, near, 0), spot(w, side, every, near, 1)
        return [remote(upper, upper, w, first, other_side), remote(lower, lower, w, first + 1, other_near)]

    def last_copies(w):
        upper, lower = spot(w, every, every, near, 0), spot(w, side, every, every, 1)
        return [remote(upper, upper, w, first + 2, other_near), remote(lower, lower, w, first + 3, other_side)]

    barrier = pltpu.get_barrier_semaphore()
    for device in [deep_peer(k) for k in range(1, deep_count)] + [other_side, other_near]:
        pl.semaphore_signal(barrier, inc=1, device_id=device, device_id_type=pl.DeviceIdType.MESH)
    pl.semaphore_wait(barrier, deep_count + 1)

    stages = [[deep_copies(w), middle_copies(w), last_copies(w)] for w in range(3)]
    local = [
        pltpu.make_async_copy(shards[w], spot(w, side, deep, near, every), local_sem.at[w]) for w in range(3)
    ]

    def start(w, stage):
        for copy in stages[w][stage]:
            copy.start()

    def arrived(w, stage):
        for copy in stages[w][stage]:
            copy.wait_recv()

    start(0, 0)
    for copy in local:
        copy.start()
    for copy in local:
        copy.wait()
    arrived(0, 0)
    start(0, 1)
    start(1, 0)
    arrived(0, 1)
    start(0, 2)
    arrived(1, 0)
    start(1, 1)
    start(2, 0)
    arrived(1, 1)
    start(1, 2)
    arrived(2, 0)
    start(2, 1)
    arrived(2, 1)
    start(2, 2)
    for w in range(3):
        arrived(w, 2)
    for w in range(3):
        for stage in range(3):
            for copy in stages[w][stage]:
                copy.wait_send()


def gather_weights(dp, packed, up, down):
    rows, cols = packed.shape
    deep_count, half = dp // 2, rows // 2
    shards = [p.reshape(2, half, cols) for p in (packed, up, down)]
    wide = jax.ShapeDtypeStruct((deep_count, 2, 2, half, 2 * cols), BF16)
    packed_full, up_full, down_full = pl.pallas_call(
        lambda *refs: gather_kernel(*refs, deep_count=deep_count),
        out_shape=(jax.ShapeDtypeStruct((2, deep_count, 2, 2, half, cols), BF16), wide, wide),
        in_specs=[pl.BlockSpec(memory_space=pltpu.VMEM)] * 3,
        out_specs=(pl.BlockSpec(memory_space=pl.ANY),) * 3,
        scratch_shapes=[
            pltpu.SemaphoreType.DMA((3,)),
            pltpu.SemaphoreType.DMA((3, deep_count + 3)),
            pltpu.SemaphoreType.DMA((3, deep_count + 3)),
        ],
        compiler_params=pltpu.CompilerParams(collective_id=0, has_side_effects=True),
        name="gather_weights",
    )(*shards)
    return (
        packed_full.reshape(2, dp * rows, cols),
        up_full.reshape(dp * rows, 2 * cols),
        down_full.reshape(dp * rows, 2 * cols),
    )


def scatter_grad(at, parts):
    cols = parts[0].shape[1]
    rows = parts[0].shape[0] // at.dp
    stacked = jnp.stack([p.reshape(at.dp // 2, 2, 2, rows // 2, cols) for p in parts])
    upper, lower = stacked[:, :, :, 0], stacked[:, :, :, 1]
    got_upper = at.swap_near(pick(1 - at.near, upper, 2))
    got_lower = at.swap_side(pick(1 - at.side, lower, 0))
    upper = pick(at.near, upper, 2).astype(F32) + got_upper.astype(F32)
    lower = pick(at.side, lower, 0).astype(F32) + got_lower.astype(F32)
    got_upper = at.swap_side(pick(1 - at.side, upper, 0).astype(BF16))
    got_lower = at.swap_near(pick(1 - at.near, lower, 1).astype(BF16))
    upper = pick(at.side, upper, 0) + got_upper.astype(F32)
    lower = pick(at.near, lower, 1) + got_lower.astype(F32)
    total = jnp.concatenate([upper, lower], axis=1)
    for bit in range(at.deep_bits):
        total = total.reshape(-1, 2, rows, cols)
        got = at.swap_deep(pick(1 - at.deep_bit(bit), total, 1).astype(BF16), bit)
        total = pick(at.deep_bit(bit), total, 1) + got.astype(F32)
    return total.reshape(rows, cols)


def body(
    layer_input,
    out_grad,
    lengths,
    entry_weight,
    query_bias,
    value_bias,
    exit_weight,
    exit_bias,
    first_gain,
    first_shift,
    up_weight,
    up_bias,
    down_weight,
    down_bias,
    second_gain,
    second_shift,
):
    at = Places(lax.axis_size("dp"), lax.axis_size("tensor"))
    own, width = layer_input.shape
    part = entry_weight.shape[2]
    hidden = up_weight.shape[1]
    shard_rows = entry_weight.shape[0]
    heads = part // HD
    scale = 1.0 / math.sqrt(HD)

    def mine(vector):
        pieces = vector.reshape(2, 2, vector.shape[0] // 4)
        return pick(at.core, pieces, 1).reshape(-1)

    def placed(local):
        pieces = local.reshape(2, 1, local.shape[0] // 2)
        empty = jnp.zeros((2, 2, local.shape[0] // 2), F32)
        return lax.dynamic_update_slice(empty, pieces, (0, at.core, 0)).reshape(-1)

    def half(rows, index):
        return lax.dynamic_slice_in_dim(rows, index * own, own, 0)

    def both(rows):
        return ordered(at.core, rows, at.swap_core(rows), 0).reshape(2 * own, rows.shape[1])

    def shared_sum(rows, weights):
        def product(index):
            return sum(against(half(r, index), w) for r, w in zip(rows, weights))

        far = at.swap_core(product(1 - at.core).astype(BF16))
        return product(at.core) + far.astype(F32)

    packed = jnp.concatenate([entry_weight.reshape(shard_rows, 3 * part), exit_weight.T], axis=1)
    packed_full, up_matrix, down_matrix = gather_weights(at.dp, packed, up_weight, down_weight.T)
    entry_sides = [packed_full[s, :, : 3 * part] for s in range(2)]
    exit_sides = [packed_full[s, :, 3 * part :] for s in range(2)]

    length = lax.dynamic_slice_in_dim(lengths, at.side, 1)
    rows_all = both(layer_input)
    query_local = mine(query_bias).reshape(2, part)
    value_local = mine(value_bias).reshape(2, part)
    mixed, context, stats = [], [], []
    for s in range(2):
        offsets = jnp.concatenate([query_local[s], jnp.zeros((part,), F32), value_local[s]])
        mixed.append((plain(rows_all, entry_sides[s]) + offsets).astype(BF16))
        piece, stat = attend(mixed[s], length, heads, scale)
        context.append(piece)
        stats.append(stat)
    attended = shared_sum(context, exit_sides)
    first_sum = layer_input.astype(F32) + attended + exit_bias
    first_unit, first_inverse = norm_parts(first_sum)
    normed = (first_unit * first_gain + first_shift).astype(BF16)

    normed_all = both(normed)
    upper = plain(normed_all, up_matrix) + mine(up_bias)
    active_full, gelu_pull = jax.vjp(lambda u: jax.nn.gelu(u, approximate=False), upper)
    active = active_full.astype(BF16)
    lowered = shared_sum([active], [down_matrix])
    second_sum = normed.astype(F32) + lowered + down_bias
    second_unit, second_inverse = norm_parts(second_sum)
    layer_output = (second_unit * second_gain + second_shift).astype(BF16)

    grad = out_grad.astype(F32)
    second_grad = norm_back(grad, second_gain, second_unit, second_inverse)
    second_gain_grad = jnp.sum(grad * second_unit, axis=0)
    second_shift_grad = jnp.sum(grad, axis=0)
    down_bias_grad = jnp.sum(second_grad, axis=0)
    lowered_all = both(second_grad.astype(BF16))
    upper_grad = gelu_pull(plain(lowered_all, down_matrix))[0].astype(BF16)
    down_partial = across(lowered_all, active).astype(BF16)
    down_grad = scatter_grad(at, [down_partial[:, :hidden], down_partial[:, hidden:]])
    up_bias_local = jnp.sum(upper_grad.astype(F32), axis=0)
    normed_grad = second_grad + shared_sum([upper_grad], [up_matrix])
    up_partial = across(normed_all, upper_grad).astype(BF16)
    up_grad = scatter_grad(at, [up_partial[:, :hidden], up_partial[:, hidden:]])

    first_grad = norm_back(normed_grad, first_gain, first_unit, first_inverse)
    first_gain_grad = jnp.sum(normed_grad * first_unit, axis=0)
    first_shift_grad = jnp.sum(normed_grad, axis=0)
    exit_bias_grad = jnp.sum(first_grad, axis=0)
    attended_all = both(first_grad.astype(BF16))
    mixed_grad, packed_parts, query_sums, value_sums = [], [], [], []
    for s in range(2):
        context_grad = plain(attended_all, exit_sides[s]).astype(BF16)
        piece = attend_back(mixed[s], context_grad, stats[s], length, heads, scale)
        mixed_grad.append(piece)
        sums = jnp.sum(piece.astype(F32), axis=0)
        query_sums.append(sums[:part])
        value_sums.append(sums[2 * part :])
        packed_parts.append(
            jnp.concatenate([across(rows_all, piece).astype(BF16), across(attended_all, context[s]).astype(BF16)], axis=1)
        )
    query_bias_local = jnp.concatenate(query_sums)
    value_bias_local = jnp.concatenate(value_sums)
    packed_grad = scatter_grad(at, packed_parts)
    input_grad = first_grad + shared_sum(mixed_grad, entry_sides)

    vectors = [
        placed(query_bias_local),
        placed(value_bias_local),
        exit_bias_grad,
        first_gain_grad,
        first_shift_grad,
        placed(up_bias_local),
        down_bias_grad,
        second_gain_grad,
        second_shift_grad,
    ]
    sizes = [v.shape[0] for v in vectors]
    total = jnp.concatenate(vectors).reshape(-1, 128)
    total = total + at.swap_core(total)
    total = total + at.swap_side(total)
    total = total + at.swap_near(total)
    for bit in range(at.deep_bits):
        total = total + at.swap_deep(total, bit)
    total = total.reshape(-1)
    sums = []
    start = 0
    for size in sizes:
        sums.append(total[start : start + size])
        start += size

    return (
        layer_output,
        input_grad,
        packed_grad[:, : 3 * part].reshape(shard_rows, 3, part),
        sums[0],
        sums[1],
        packed_grad[:, 3 * part :].T,
        sums[2],
        sums[3],
        sums[4],
        up_grad,
        sums[5],
        down_grad.T,
        sums[6],
        sums[7],
        sums[8],
    )


def solution(mesh):
    rows = P(("dp", "tensor"), None)
    return jax.shard_map(
        body,
        mesh=mesh,
        in_specs=(
            rows,
            rows,
            P("dp"),
            P("dp", None, "tensor"),
            P(),
            P(),
            P("tensor", "dp"),
            P(),
            P(),
            P(),
            P("dp", "tensor"),
            P(),
            P("tensor", "dp"),
            P(),
            P(),
            P(),
        ),
        out_specs=(
            rows,
            rows,
            P("dp", None, "tensor"),
            P(),
            P(),
            P("tensor", "dp"),
            P(),
            P(),
            P(),
            P("dp", "tensor"),
            P(),
            P("tensor", "dp"),
            P(),
            P(),
            P(),
        ),
        check_vma=False,
    )
```
